256 devices in a mesh: lat: 16 (over x, y), lon: 16 (over z, core).
Axes of the slice: x: 4, y: 4, z: 8, core: 2. Of those that a mesh axis runs over, the one named last changes fastest.
Arguments:
- transport: bfloat16 [48, 2048, 6144], P(None, 'lat', 'lon'), may hold values from -0.046875 to 0.046875
- sigma_class: int32 [48, 2048, 6144], P(None, 'lat', 'lon'), may hold values from 0 to 199
- basin_id: int32 [2048, 6144], P('lat', 'lon'), may hold values from 0 to 3
- depth_levels: int32 [2048, 6144], P('lat', 'lon'), may hold values from 0 to 48
Outputs:
- overturning: bfloat16 [4, 200, 2048], replicated
The draws below stay inside these ranges and needn't reach their ends.
Inputs may be any that keep to these rules, and one draw needn't show every extreme that they name: `depth_levels`: 0 marks a land column.
All inputs are finite; a program needn't handle non-finite values.
Results may differ from the reference program's by a relative error of at most 0.001.
Values may be sent and summed in bfloat16 or wider, within the bound.
A program may use at most 64 MiB of HBM per device.

```python
import jax
import jax.numpy as jnp
from jax import lax

CLASSES = 200
BASINS = 4
ROWS_DEV = 128
COLS_DEV = 384
LEVELS = 48
NJ = 2048
NI = 6144
N_LON = 16


def touch_ends(values, own_key, low, high):
    longest = values.shape.index(max(values.shape))
    spots = []
    for shift in (0, 1):
        where = [jax.random.randint(jax.random.fold_in(own_key, axis), (), 0, length) for axis, length in enumerate(values.shape)]
        where[longest] = (where[longest] + shift) % values.shape[longest]
        spots.append(tuple(where))
    return values.at[spots[0]].set(low).at[spots[1]].set(high)


def steps_of(key, dims, cuts, low, largest):
    def one(dim, shards_of):
        draws = jax.random.uniform(jax.random.fold_in(jax.random.fold_in(key, 6), dim), (shards_of,), jnp.float32, low / len(cuts), largest / len(cuts))
        return jnp.repeat(jnp.exp(draws), dims[dim] // shards_of).reshape((-1,) + (1,) * (len(dims) - dim - 1))

    factor_of = one(*cuts[0])
    for cut in cuts[1:]:
        factor_of = factor_of * one(*cut)
    return factor_of


def bell_draw(key, extent, deviation, reach, split=(), held_as=jnp.bfloat16):
    result = jax.random.normal(key, extent, jnp.float32) * deviation
    if len(split) > 0:
        result = steps_of(key, extent, split, -0.22, 0.18) * result
    return jnp.clip(result, min=-reach, max=reach).astype(held_as)


def setup_inputs(seed: int = 0) -> dict:
    key_of = jax.random.split(jax.random.key(seed), 5)
    return {
        "transport": bell_draw(key_of[0], (LEVELS, NJ, NI), (2.0 / (COLS_DEV * N_LON * LEVELS / BASINS) ** 0.5), 0.046875, ((1, 16), (2, 16))),
        "sigma_class": touch_ends(jax.random.randint(key_of[1], (LEVELS, NJ, NI), 0, CLASSES), jax.random.fold_in(key_of[1], 1), 0, CLASSES - 1).astype(jnp.int32),
        "basin_id": touch_ends(jax.random.randint(key_of[2], (NJ, NI), 0, BASINS), jax.random.fold_in(key_of[2], 1), 0, BASINS - 1).astype(jnp.int32),
        "depth_levels": touch_ends(jax.random.randint(key_of[3], (NJ, NI), 0, LEVELS + 1), jax.random.fold_in(key_of[3], 1), 0, LEVELS).astype(jnp.int32),
    }


def bin_block(transport, sigma_class, basin_id, depth_levels):
    depth_count, row_count, col_count = sigma_class.shape
    level_index = lax.broadcasted_iota(jnp.int32, (depth_count, row_count, col_count), 0)
    row_index = lax.broadcasted_iota(jnp.int32, (depth_count, row_count, col_count), 1)
    wet_cells = level_index < depth_levels[None, :, :]
    weights = jnp.where(wet_cells, transport.astype(jnp.float32), jnp.float32(0.0))
    bin_index = ((basin_id[None, :, :] * CLASSES + sigma_class) * row_count + row_index).astype(jnp.int32)
    flat = jax.ops.segment_sum(weights.reshape(-1), bin_index.reshape(-1), num_segments=BASINS * CLASSES * row_count)
    return flat.reshape(BASINS, CLASSES, row_count)


def reference(transport, sigma_class, basin_id, depth_levels):
    block_count = NJ // ROWS_DEV

    def one_block(start):
        return bin_block(
            lax.dynamic_slice_in_dim(transport, start, ROWS_DEV, 1),
            lax.dynamic_slice_in_dim(sigma_class, start, ROWS_DEV, 1),
            lax.dynamic_slice_in_dim(basin_id, start, ROWS_DEV, 0),
            lax.dynamic_slice_in_dim(depth_levels, start, ROWS_DEV, 0),
        )

    starts = (jnp.arange(block_count) * ROWS_DEV).astype(jnp.int32)
    tables = lax.map(one_block, starts)
    table = jnp.transpose(tables, (1, 2, 0, 3)).reshape(BASINS, CLASSES, NJ)
    return jnp.cumsum(table, axis=1).astype(jnp.bfloat16)
```

```python
import functools

import jax
import jax.numpy as jnp
from jax import lax
from jax.experimental import pallas as pl
from jax.experimental.pallas import tpu as pltpu
from jax.sharding import PartitionSpec as P

CLASSES = 200
BASINS = 4
LOW = 32
HIGH = 7
SUB = 8
PER_STEP = 4
LANES = 128


def one_hot_kernel(flow_ref, class_ref, basin_ref, depth_ref, out_ref):
    levels, rows, cols = class_ref.shape
    tiles = cols // LANES
    m = BASINS * HIGH * SUB
    n = LOW * SUB

    def twice(x):
        return jnp.concatenate([x, x - 1.0], axis=0).astype(jnp.bfloat16)

    def run(*accs):
        def step(s, _):
            for sub in range(rows // SUB):
                r = pl.ds(sub * SUB, SUB)
                pieces = []
                for level in range(PER_STEP):
                    k = s * PER_STEP + level
                    for tile in range(tiles):
                        pieces.append((k, pl.ds(tile * LANES, LANES)))
                halves = []
                for index, (k, c) in enumerate(pieces):
                    klass = class_ref[k, r, c]
                    high = basin_ref[r, c] * HIGH + (klass >> 5)
                    wet = k < depth_ref[r, c]
                    high = jnp.where(wet, high, -100)
                    low = klass & (LOW - 1)
                    flow = flow_ref[k, r, c].astype(jnp.float32)
                    halves.append((
                        twice(high.astype(jnp.float32)),
                        twice(low.astype(jnp.float32)),
                        jnp.concatenate([flow, flow], axis=0).astype(jnp.bfloat16),
                    ))
                    if len(halves) < 2:
                        continue
                    high2, low2, flow2 = [jnp.concatenate(h, axis=1) for h in zip(*halves)]
                    halves = []
                    zero = jnp.zeros_like(flow2)
                    one = jnp.ones_like(flow2)
                    rhs = jnp.concatenate(
                        [jnp.where(low2 == jnp.bfloat16(2 * u), one, zero) for u in range(LOW // 2)], axis=0
                    )
                    lhs = jnp.concatenate(
                        [jnp.where(high2 == jnp.bfloat16(2 * t), flow2, zero) for t in range(BASINS * HIGH // 2)], axis=0
                    )
                    q = (index // 2) % 2
                    reg = (index // 4) % 2
                    pltpu.matmul_push_rhs(rhs, staging_register=reg, mxu_index=q, transpose=True)
                    pltpu.matmul_acc_lhs(accs[2 * sub + q], lhs, load_staged_rhs=reg)
            return 0

        lax.fori_loop(0, levels // PER_STEP, step, 0)
        row = lax.broadcasted_iota(jnp.int32, (1, SUB, n), 1)
        col = lax.broadcasted_iota(jnp.int32, (1, SUB, n), 2)
        own = (col % SUB) == row
        for sub in range(rows // SUB):
            both = pltpu.matmul_pop(accs[2 * sub]) + pltpu.matmul_pop(accs[2 * sub + 1])
            cube = both.reshape(m // SUB, SUB, n)
            out_ref[sub] = jnp.sum(jnp.where(own, cube, 0.0), axis=1)

    accs = [pltpu.ACC(q)((m, n), jnp.float32) for _ in range(rows // SUB) for q in range(2)]
    pl.run_scoped(run, *accs)


def bin_rows(transport, sigma_class, basin_id, depth_levels):
    levels, rows, cols = sigma_class.shape
    step_rows = 2 * SUB
    groups = rows // SUB
    return pl.pallas_call(
        one_hot_kernel,
        grid=(rows // step_rows,),
        in_specs=[
            pl.BlockSpec((levels, step_rows, cols), lambda g: (0, g, 0)),
            pl.BlockSpec((levels, step_rows, cols), lambda g: (0, g, 0)),
            pl.BlockSpec((step_rows, cols), lambda g: (g, 0)),
            pl.BlockSpec((step_rows, cols), lambda g: (g, 0)),
        ],
        out_specs=pl.BlockSpec((2, BASINS * HIGH, LOW * SUB), lambda g: (g, 0, 0)),
        out_shape=jax.ShapeDtypeStruct((groups, BASINS * HIGH, LOW * SUB), jnp.float32),
        compiler_params=pltpu.CompilerParams(dimension_semantics=("arbitrary",)),
    )(transport, sigma_class, basin_id, depth_levels)


def body(transport, sigma_class, basin_id, depth_levels):
    table = bin_rows(transport, sigma_class, basin_id, depth_levels)
    table = lax.psum_scatter(table, "lon", scatter_dimension=0, tiled=True)[0]
    table = table.reshape(BASINS, HIGH * LOW, SUB)[:, :CLASSES]
    overturn = jnp.cumsum(table, axis=1).astype(jnp.bfloat16)
    return lax.all_gather(overturn, ("lat", "lon"), axis=2, tiled=True)


def solution(mesh):
    placed = (P(None, "lat", "lon"), P(None, "lat", "lon"), P("lat", "lon"), P("lat", "lon"))

    def run(*args):
        return jax.shard_map(body, mesh=mesh, in_specs=placed, out_specs=P(), check_vma=False)(*args)

    return run
```

```python
import functools

import jax
import jax.numpy as jnp
from jax import lax
from jax.experimental import pallas as pl
from jax.experimental.pallas import tpu as pltpu
from jax.sharding import PartitionSpec as P

CLASSES = 200
BASINS = 4
LOW = 32
HIGH = 7
SUB = 8
PER_STEP = 4
LANES = 128


def one_hot_kernel(flow_ref, class_ref, basin_ref, depth_ref, out_ref):
    levels, rows, cols = class_ref.shape
    tiles = cols // LANES
    m = BASINS * HIGH * SUB
    n = LOW * SUB

    def twice(x):
        return jnp.concatenate([x, x - 1.0], axis=0).astype(jnp.bfloat16)

    def run(*accs):
        def step(s, _):
            for sub in range(rows // SUB):
                r = pl.ds(sub * SUB, SUB)
                pieces = []
                for level in range(PER_STEP):
                    k = s * PER_STEP + level
                    for tile in range(tiles):
                        pieces.append((k, pl.ds(tile * LANES, LANES)))
                halves = []
                for index, (k, c) in enumerate(pieces):
                    klass = class_ref[k, r, c]
                    high = basin_ref[r, c] * HIGH + (klass >> 5)
                    wet = k < depth_ref[r, c]
                    high = jnp.where(wet, high, -100)
                    low = klass & (LOW - 1)
                    flow = flow_ref[k, r, c].astype(jnp.float32)
                    halves.append((
                        twice(high.astype(jnp.float32)),
                        twice(low.astype(jnp.float32)),
                        jnp.concatenate([flow, flow], axis=0).astype(jnp.bfloat16),
                    ))
                    if len(halves) < 2:
                        continue
                    high2, low2, flow2 = [jnp.concatenate(h, axis=1) for h in zip(*halves)]
                    halves = []
                    zero = jnp.zeros_like(flow2)
                    one = jnp.ones_like(flow2)
                    rhs = jnp.concatenate(
                        [jnp.where(low2 <= jnp.bfloat16(2 * u), one, zero) for u in range(LOW // 2)], axis=0
                    )
                    lhs = jnp.concatenate(
                        [jnp.where(high2 == jnp.bfloat16(2 * t), flow2, zero) for t in range(BASINS * HIGH // 2)], axis=0
                    )
                    q = (index // 2) % 2
                    reg = (index // 4) % 2
                    pltpu.matmul_push_rhs(rhs, staging_register=reg, mxu_index=q, transpose=True)
                    pltpu.matmul_acc_lhs(accs[2 * sub + q], lhs, load_staged_rhs=reg)
            return 0

        lax.fori_loop(0, levels // PER_STEP, step, 0)
        row = lax.broadcasted_iota(jnp.int32, (1, SUB, n), 1)
        col = lax.broadcasted_iota(jnp.int32, (1, SUB, n), 2)
        own = (col % SUB) == row
        lane = lax.broadcasted_iota(jnp.int32, (BASINS * HIGH, LANES), 1)
        for sub in range(rows // SUB):
            group = pl.program_id(0) * (rows // SUB) + sub
            both = pltpu.matmul_pop(accs[2 * sub]) + pltpu.matmul_pop(accs[2 * sub + 1])
            cube = both.reshape(m // SUB, SUB, n)
            part = jnp.sum(jnp.where(own, cube, 0.0), axis=1)
            whole = jnp.where(lane >= LANES - SUB, part[:, n - LANES :], 0.0)
            for shift in (SUB, 2 * SUB, 4 * SUB, 8 * SUB):
                whole = whole + pltpu.roll(whole, shift, 1)
            for basin in range(BASINS):
                before = jnp.zeros((1, LANES), jnp.float32)
                for digit in range(HIGH):
                    h = basin * HIGH + digit
                    for half in range(n // LANES):
                        out_ref[h, half, pl.ds(group, 1), :] = (
                            part[h : h + 1, half * LANES : (half + 1) * LANES] + before
                        )
                    before = before + whole[h : h + 1]

    accs = [pltpu.ACC(q)((m, n), jnp.float32) for _ in range(rows // SUB) for q in range(2)]
    pl.run_scoped(run, *accs)


def bin_rows(transport, sigma_class, basin_id, depth_levels):
    levels, rows, cols = sigma_class.shape
    step_rows = 2 * SUB
    groups = rows // SUB
    shape = (BASINS * HIGH, LOW * SUB // LANES, groups, LANES)
    return pl.pallas_call(
        one_hot_kernel,
        grid=(rows // step_rows,),
        in_specs=[
            pl.BlockSpec((levels, step_rows, cols), lambda g: (0, g, 0)),
            pl.BlockSpec((levels, step_rows, cols), lambda g: (0, g, 0)),
            pl.BlockSpec((step_rows, cols), lambda g: (g, 0)),
            pl.BlockSpec((step_rows, cols), lambda g: (g, 0)),
        ],
        out_specs=pl.BlockSpec(shape, lambda g: (0, 0, 0, 0)),
        out_shape=jax.ShapeDtypeStruct(shape, jnp.float32),
        compiler_params=pltpu.CompilerParams(dimension_semantics=("arbitrary",)),
    )(transport, sigma_class, basin_id, depth_levels)


def spread_kernel(
    n_lat, n_lon, side, table_ref, out_ref, parts, shuffle,
    sum_send, sum_recv, z_send, z_recv, one_send, one_recv, two_send, two_recv, pair_send, pair_recv,
):
    owners, size, _ = table_ref.shape
    chunks = owners // 2
    lat, lon = lax.axis_index("lat"), lax.axis_index("lon")
    x, y = lat // side, lax.rem(lat, side)
    z, core = lon // 2, lax.rem(lon, 2)
    depth = n_lon // 2

    def at(to_lat, to_lon):
        return {"lat": to_lat, "lon": to_lon}

    def along(axis, d):
        if axis == 0:
            return lax.rem(x + d, side) * side + y
        return x * side + lax.rem(y + d, side)

    def block(chunk, of_lat):
        rows = pl.ds(pl.multiple_of((2 * chunk + core) * size, size), size)
        return out_ref.at[rows, pl.ds(pl.multiple_of(of_lat * LANES, LANES), LANES)]

    def send(src, dst, send_sem, recv_sem, to):
        copy = pltpu.make_async_remote_copy(
            src_ref=src, dst_ref=dst, send_sem=send_sem, recv_sem=recv_sem,
            device_id=to, device_id_type=pl.DeviceIdType.MESH,
        )
        return copy

    barrier = pltpu.get_barrier_semaphore()
    for d in range(1, n_lon):
        pl.semaphore_signal(barrier, inc=1, device_id=at(lat, lax.rem(lon + d, n_lon)), device_id_type=pl.DeviceIdType.MESH)
    for axis in range(2):
        for d in range(1, side):
            pl.semaphore_signal(barrier, inc=1, device_id=at(along(axis, d), lon), device_id_type=pl.DeviceIdType.MESH)
    pl.semaphore_wait(barrier, n_lon - 1 + 2 * (side - 1))

    def share(d):
        to = lax.rem(lon + d, n_lon)
        return to, send(table_ref.at[lax.rem(to, owners)], parts.at[d - 1], sum_send.at[d - 1], sum_recv.at[d - 1], at(lat, to))

    for d in range(1, n_lon):
        to, copy = share(d)

        @pl.when(to < owners)
        def _():
            copy.start()

    groups = LANES // SUB
    line = lax.broadcasted_iota(jnp.int32, (LANES, LANES), 0)
    lane = lax.broadcasted_iota(jnp.int32, (LANES, LANES), 1) % SUB
    for low in range(groups):
        shuffle[:, low * LANES : (low + 1) * LANES] = jnp.where(line == lane + low * SUB, 1.0, 0.0).astype(jnp.bfloat16)

    partner = at(lat, z * 2 + 1 - core)

    def to_pair(chunk, of_lat):
        send(block(chunk, of_lat), block(chunk, of_lat), pair_send, pair_recv, partner).start()

    @pl.when(lon < owners)
    def _():
        total = table_ref[lax.rem(lon, owners)]
        for d in range(1, n_lon):
            share(d)[1].wait_recv()
            total = total + parts[d - 1]
        wide = jnp.dot(total.astype(jnp.bfloat16), shuffle[...], preferred_element_type=jnp.float32)
        row = lax.broadcasted_iota(jnp.int32, (size // groups, groups, LANES), 1)
        col = lax.broadcasted_iota(jnp.int32, (size // groups, groups, LANES), 2)
        own = row == col // SUB
        lines = []
        for low in range(groups):
            piece = wide[:, low * LANES : (low + 1) * LANES].reshape(size // groups, groups, LANES)
            lines.append(jnp.sum(jnp.where(own, piece, 0.0), axis=1, keepdims=True))
        mine = jnp.concatenate(lines, axis=1).reshape(size, LANES)
        block(z, lat)[...] = mine.astype(jnp.bfloat16)
        for d in range(1, depth):
            to = lax.rem(z + d, depth) * 2 + core
            send(block(z, lat), block(z, lat), z_send.at[d - 1], z_recv.at[z], at(lat, to)).start()

    def first(chunk, d):
        return send(block(chunk, lat), block(chunk, lat), one_send.at[chunk, d - 1], one_recv.at[chunk, d - 1],
                    at(along(chunk % 2, d), lon))

    def second(chunk, of, of_lat, d):
        return send(block(chunk, of_lat), block(chunk, of_lat), two_send, two_recv.at[chunk, of, d - 1],
                    at(along(1 - chunk % 2, d), lon))

    def came(chunk, d):
        return along(chunk % 2, side - d)

    def came_twice(chunk, of, d):
        if chunk % 2 == 0:
            return lax.rem(x + (side - of), side) * side + lax.rem(y + (side - d), side)
        return lax.rem(x + (side - d), side) * side + lax.rem(y + (side - of), side)

    for chunk in range(chunks):

        @pl.when(z != chunk)
        def _():
            send(block(chunk, lat), block(chunk, lat), z_send.at[0], z_recv.at[chunk], at(lat, lon)).wait_recv()

        for d in range(1, side):
            first(chunk, d).start()
        for d in range(1, side):
            second(chunk, 0, lat, d).start()
        to_pair(chunk, lat)
    for chunk in range(chunks):
        for of in range(1, side):
            first(chunk, of).wait_recv()
            for d in range(1, side):
                second(chunk, of, came(chunk, of), d).start()
            to_pair(chunk, came(chunk, of))
    for chunk in range(chunks):
        for of in range(side):
            for d in range(1, side):
                second(chunk, of, lat, d).wait_recv()
                to_pair(chunk, came_twice(chunk, of, d))

    for d in range(1, n_lon):
        to, copy = share(d)

        @pl.when(to < owners)
        def _():
            copy.wait_send()

    @pl.when(lon < owners)
    def _():
        for d in range(1, depth):
            send(block(z, lat), block(z, lat), z_send.at[d - 1], z_recv.at[z], at(lat, lon)).wait_send()

    for chunk in range(chunks):
        for d in range(1, side):
            first(chunk, d).wait_send()
    seconds = out_ref.at[pl.ds(0, chunks * side * (side - 1) * size // n_lat)]
    pltpu.make_async_copy(seconds, seconds, two_send).wait()
    half = out_ref.at[pl.ds(0, chunks * size)]
    pltpu.make_async_copy(half, half, pair_send).wait()
    pltpu.make_async_copy(half, half, pair_recv).wait()


def spread(table, n_lat, n_lon):
    owners, size, _ = table.shape
    side = 4
    chunks = owners // 2
    dma = pltpu.SemaphoreType.DMA
    return pl.pallas_call(
        functools.partial(spread_kernel, n_lat, n_lon, side),
        out_shape=jax.ShapeDtypeStruct((owners * size, n_lat * LANES), jnp.bfloat16),
        in_specs=[pl.BlockSpec(memory_space=pltpu.VMEM)],
        out_specs=pl.BlockSpec(memory_space=pltpu.VMEM),
        scratch_shapes=[
            pltpu.VMEM((n_lon - 1, size, LANES), jnp.float32),
            pltpu.VMEM((LANES, LANES // SUB * LANES), jnp.bfloat16),
            dma((n_lon - 1,)), dma((n_lon - 1,)),
            dma((n_lon // 2 - 1,)), dma((chunks,)),
            dma((chunks, side - 1)), dma((chunks, side - 1)),
            dma, dma((chunks, side, side - 1)),
            dma, dma,
        ],
        compiler_params=pltpu.CompilerParams(collective_id=0, has_side_effects=True),
    )(table)


def body(n_lat, n_lon, transport, sigma_class, basin_id, depth_levels):
    table = bin_rows(transport, sigma_class, basin_id, depth_levels)
    groups = table.shape[2]
    table = table.reshape(BASINS * HIGH * 2 // 4, 4 * groups, LANES)
    overturn = spread(table, n_lat, n_lon)
    return overturn.reshape(BASINS, HIGH * LOW, -1)[:, :CLASSES]


def solution(mesh):
    placed = (P(None, "lat", "lon"), P(None, "lat", "lon"), P("lat", "lon"), P("lat", "lon"))
    run = functools.partial(body, mesh.shape["lat"], mesh.shape["lon"])
    return jax.shard_map(run, mesh=mesh, in_specs=placed, out_specs=P(), check_vma=False)
```

```python
import functools

import jax
import jax.numpy as jnp
from jax import lax
from jax.experimental import pallas as pl
from jax.experimental.pallas import tpu as pltpu
from jax.sharding import PartitionSpec as P

CLASSES = 200
BASINS = 4
LOW = 32
HIGH = 7
SUB = 8
LANES = 128
SHARE = 4
PHASE = 4
SIDE = 4
MESH = pl.DeviceIdType.MESH


def overturn_kernel(
    n_lat, n_lon, flow_ref, class_ref, basin_ref, depth_ref, out_ref,
    table, parts, shuffle, lines, land,
    sum_send, sum_recv, z_send, z_recv, one_send, one_recv, two_send, two_recv, pair_send, pair_recv, out_sem,
):
    levels, rows, cols = class_ref.shape
    tiles = cols // LANES
    m = BASINS * HIGH * SUB
    n = LOW * SUB
    groups = LANES // SUB
    step = pl.program_id(0)
    steps = pl.num_programs(0)
    phases, owners, size, _ = table.shape
    chunk_rows = phases * size
    chunks = owners // 2
    depth = n_lon // 2
    lat, lon = lax.axis_index("lat"), lax.axis_index("lon")
    x, y = lat // SIDE, lax.rem(lat, SIDE)
    z, core = lon // 2, lax.rem(lon, 2)

    def at(to_lat, to_lon):
        return {"lat": to_lat, "lon": to_lon}

    def along(axis, d):
        if axis == 0:
            return lax.rem(x + d, SIDE) * SIDE + y
        return x * SIDE + lax.rem(y + d, SIDE)

    def block(chunk, of_lat):
        lines_of = pl.ds(pl.multiple_of((2 * chunk + core) * chunk_rows, chunk_rows), chunk_rows)
        return land.at[lines_of, pl.ds(pl.multiple_of(of_lat * LANES, LANES), LANES)]

    def send(src, dst, send_sem, recv_sem, to):
        return pltpu.make_async_remote_copy(
            src_ref=src, dst_ref=dst, send_sem=send_sem, recv_sem=recv_sem, device_id=to, device_id_type=MESH
        )

    barrier = pltpu.get_barrier_semaphore()

    @pl.when(step == 0)
    def _():
        for d in range(1, n_lon):
            pl.semaphore_signal(barrier, inc=1, device_id=at(lat, lax.rem(lon + d, n_lon)), device_id_type=MESH)
        for axis in range(2):
            for d in range(1, SIDE):
                pl.semaphore_signal(barrier, inc=1, device_id=at(along(axis, d), lon), device_id_type=MESH)
        line = lax.broadcasted_iota(jnp.int32, (LANES, LANES), 0)
        lane = lax.broadcasted_iota(jnp.int32, (LANES, LANES), 1) & (SUB - 1)
        for low in range(groups):
            at_low = pl.ds(low * LANES, LANES)
            shuffle[:LANES, at_low] = jnp.where(line == lane + low * SUB, 1.0, 0.0).astype(jnp.bfloat16)
            shuffle[LANES:, at_low] = jnp.zeros((LANES, LANES), jnp.bfloat16)
        pl.semaphore_wait(barrier, n_lon - 1 + 2 * (SIDE - 1))


    def twice(v):
        return jnp.concatenate([v, v - 1.0], axis=0).astype(jnp.bfloat16)

    digit = lax.broadcasted_iota(jnp.int32, (2 * LANES, LANES), 1) // (2 * SUB) * 2
    limits = [
        (digit + part * (LANES // SUB)).astype(jnp.float32).astype(jnp.bfloat16) for part in range(n // LANES)
    ]

    def add_products(sub, accs):
        r = pl.ds(sub * SUB, SUB)
        base = [basin_ref[r, pl.ds(tile * LANES, LANES)] * HIGH for tile in range(tiles)]
        wet_levels = [depth_ref[r, pl.ds(tile * LANES, LANES)] for tile in range(tiles)]
        halves = []
        for index in range(levels * tiles):
            k, tile = index // tiles, index % tiles
            c = pl.ds(tile * LANES, LANES)
            klass = class_ref[k, r, c]
            high = jnp.where(k < wet_levels[tile], base[tile] + (klass >> 5), -100)
            low = klass & (LOW - 1)
            flow = flow_ref[k, r, c].astype(jnp.float32)
            halves.append((
                twice(high.astype(jnp.float32)),
                twice(low.astype(jnp.float32)),
                jnp.concatenate([flow, flow], axis=0).astype(jnp.bfloat16),
            ))
            if len(halves) < 2:
                continue
            high2, low2, flow2 = [jnp.concatenate(h, axis=1) for h in zip(*halves)]
            halves = []
            zero = jnp.zeros_like(flow2)
            wide = jnp.concatenate([low2] * (LANES // (2 * SUB)), axis=0).T
            one = jnp.ones_like(wide)
            none = jnp.zeros_like(wide)
            rhs = jnp.concatenate([jnp.where(wide <= limit, one, none) for limit in limits], axis=1)
            lhs = jnp.concatenate(
                [jnp.where(high2 == jnp.bfloat16(2 * t), flow2, zero) for t in range(BASINS * HIGH // 2)], axis=0
            )
            q = (index // 2) % 2
            reg = (index // 4) % 2
            pltpu.matmul_push_rhs(rhs, staging_register=reg, mxu_index=q, transpose=False)
            pltpu.matmul_acc_lhs(accs[q], lhs, load_staged_rhs=reg)

    def finish(group, accs):
        row = lax.broadcasted_iota(jnp.int32, (1, SUB, n), 1)
        col = lax.broadcasted_iota(jnp.int32, (1, SUB, n), 2)
        own = (col & (SUB - 1)) == row
        lane = lax.broadcasted_iota(jnp.int32, (BASINS * HIGH, LANES), 1)
        both = pltpu.matmul_pop(accs[0]) + pltpu.matmul_pop(accs[1])
        part = jnp.sum(jnp.where(own, both.reshape(m // SUB, SUB, n), 0.0), axis=1)
        whole = jnp.where(lane >= LANES - SUB, part[:, n - LANES :], 0.0)
        for shift in (SUB, 2 * SUB, 4 * SUB, 8 * SUB):
            whole = whole + pltpu.roll(whole, shift, 1)
        for basin in range(BASINS):
            before = jnp.zeros((1, LANES), jnp.float32)
            for digit in range(HIGH):
                h = basin * HIGH + digit
                for half in range(n // LANES):
                    owner, share = (2 * h + half) // SHARE, (2 * h + half) % SHARE
                    table[group // PHASE, owner, pl.ds((group & (PHASE - 1)) * SHARE + share, 1), :] = (
                        part[h : h + 1, half * LANES : (half + 1) * LANES] + before
                    )
                before = before + whole[h : h + 1]


    def share_of(phase, d):
        to = lax.rem(lon + d, n_lon)
        return to, send(
            table.at[phase, lax.rem(to, owners)], parts.at[d - 1, phase],
            sum_send.at[phase, d - 1], sum_recv.at[phase, d - 1], at(lat, to),
        )

    def send_phase(phase):
        for d in range(1, n_lon):
            to, copy = share_of(phase, d)

            @pl.when(to < owners)
            def _():
                copy.start()

    def run(even, odd, moved):
        last = steps * 2
        add_products(0, even)
        finish((2 * step + last - 1) & (last - 1), odd)

        @pl.when((step > 0) & ((step & 1) == 0))
        def _():
            send_phase(step // 2 - 1)

        add_products(1, odd)
        finish(2 * step, even)

        @pl.when(step == steps - 1)
        def _():
            finish(last - 1, odd)
            send_phase(phases - 1)
            exchange(moved)


    def exchange(moved):
        partner = at(lat, z * 2 + 1 - core)

        def to_pair(chunk, of_lat):
            send(block(chunk, of_lat), block(chunk, of_lat), pair_send, pair_recv, partner).start()

        @pl.when(lon < owners)
        def _():
            totals = []
            for phase in range(phases):
                total = table[phase, lax.rem(lon, owners)]
                for d in range(1, n_lon):
                    share_of(phase, d)[1].wait_recv()
                    total = total + parts[d - 1, phase]
                totals.append(total)
            total = jnp.concatenate(totals, axis=0).astype(jnp.bfloat16)
            lhs = jnp.concatenate([total, jnp.zeros_like(total)], axis=1)
            row = lax.broadcasted_iota(jnp.int32, (chunk_rows, LANES), 0) // SHARE
            own = row == lax.broadcasted_iota(jnp.int32, (chunk_rows, LANES), 1) // SUB
            for piece in range(groups // 2):
                q = piece % 2
                pltpu.matmul_push_rhs(
                    shuffle[:, pl.ds(piece * 2 * LANES, 2 * LANES)], staging_register=0, mxu_index=q
                )
                pltpu.matmul_acc_lhs(moved[piece], lhs, load_staged_rhs=0)
            for piece in range(groups // 2):
                both = pltpu.matmul_pop(moved[piece])
                for half in range(2):
                    kept = jnp.where(own, both[:, half * LANES : (half + 1) * LANES], 0.0)
                    kept = jnp.sum(kept.reshape(chunk_rows // SUB, SUB, LANES), axis=0)
                    kept = kept[:SHARE] + kept[SHARE:]
                    for share in range(SHARE):
                        at_line = share * groups + piece * 2 + half
                        lines[at_line : at_line + 1, :] = kept[share : share + 1]
            block(z, lat)[...] = lines[...].astype(jnp.bfloat16)
            for d in range(1, depth):
                to = lax.rem(z + d, depth) * 2 + core
                send(block(z, lat), block(z, lat), z_send.at[d - 1], z_recv.at[z], at(lat, to)).start()

        def first(chunk, d):
            return send(block(chunk, lat), block(chunk, lat), one_send.at[chunk, d - 1], one_recv.at[chunk, d - 1],
                        at(along(chunk % 2, d), lon))

        def second(chunk, of, of_lat, d):
            return send(block(chunk, of_lat), block(chunk, of_lat), two_send, two_recv.at[chunk, of, d - 1],
                        at(along(1 - chunk % 2, d), lon))

        def came(chunk, d):
            return along(chunk % 2, SIDE - d)

        def came_twice(chunk, of, d):
            if chunk % 2 == 0:
                return lax.rem(x + (SIDE - of), SIDE) * SIDE + lax.rem(y + (SIDE - d), SIDE)
            return lax.rem(x + (SIDE - d), SIDE) * SIDE + lax.rem(y + (SIDE - of), SIDE)

        for chunk in range(chunks):

            @pl.when(z != chunk)
            def _():
                send(block(chunk, lat), block(chunk, lat), z_send.at[0], z_recv.at[chunk], at(lat, lon)).wait_recv()

            for d in range(1, SIDE):
                first(chunk, d).start()
            for d in range(1, SIDE):
                second(chunk, 0, lat, d).start()
            to_pair(chunk, lat)
        for chunk in range(chunks):
            for of in range(1, SIDE):
                first(chunk, of).wait_recv()
                for d in range(1, SIDE):
                    second(chunk, of, came(chunk, of), d).start()
                to_pair(chunk, came(chunk, of))
        for chunk in range(chunks):
            for of in range(SIDE):
                for d in range(1, SIDE):
                    second(chunk, of, lat, d).wait_recv()
                    to_pair(chunk, came_twice(chunk, of, d))

        half = land.at[pl.ds(0, chunks * chunk_rows)]
        pltpu.make_async_copy(half, half, pair_recv).wait()
        out = pltpu.make_async_copy(land, out_ref, out_sem)
        out.start()
        for phase in range(phases):
            for d in range(1, n_lon):
                to, copy = share_of(phase, d)

                @pl.when(to < owners)
                def _():
                    copy.wait_send()

        @pl.when(lon < owners)
        def _():
            for d in range(1, depth):
                send(block(z, lat), block(z, lat), z_send.at[d - 1], z_recv.at[z], at(lat, lon)).wait_send()

        for chunk in range(chunks):
            for d in range(1, SIDE):
                first(chunk, d).wait_send()
        seconds = land.at[pl.ds(0, chunks * SIDE * (SIDE - 1) * chunk_rows // n_lat)]
        pltpu.make_async_copy(seconds, seconds, two_send).wait()
        pltpu.make_async_copy(half, half, pair_send).wait()
        out.wait()

    def acc(q, lines_of):
        return pltpu.ACC(q)((lines_of, n), jnp.float32)

    pl.run_scoped(
        run,
        tuple(acc(q, m) for q in range(2)),
        tuple(acc(q, m) for q in range(2)),
        tuple(acc(piece % 2, chunk_rows) for piece in range(groups // 2)),
    )


def body(n_lat, n_lon, transport, sigma_class, basin_id, depth_levels):
    levels, rows, cols = sigma_class.shape
    step_rows = 2 * SUB
    owners = BASINS * HIGH * LOW * SUB // LANES // SHARE
    chunks = owners // 2
    phases = rows // SUB // PHASE
    size = SHARE * PHASE
    dma = pltpu.SemaphoreType.DMA
    everything = (owners * phases * size, n_lat * LANES)
    overturn = pl.pallas_call(
        functools.partial(overturn_kernel, n_lat, n_lon),
        grid=(rows // step_rows,),
        in_specs=[
            pl.BlockSpec((levels, step_rows, cols), lambda g: (0, g, 0)),
            pl.BlockSpec((levels, step_rows, cols), lambda g: (0, g, 0)),
            pl.BlockSpec((step_rows, cols), lambda g: (g, 0)),
            pl.BlockSpec((step_rows, cols), lambda g: (g, 0)),
        ],
        out_specs=pl.BlockSpec(memory_space=pl.ANY),
        out_shape=jax.ShapeDtypeStruct(everything, jnp.bfloat16),
        scratch_shapes=[
            pltpu.VMEM((phases, owners, size, LANES), jnp.float32),
            pltpu.VMEM((n_lon - 1, phases, size, LANES), jnp.float32),
            pltpu.VMEM((2 * LANES, LANES // SUB * LANES), jnp.bfloat16),
            pltpu.VMEM((phases * size, LANES), jnp.float32),
            pltpu.VMEM(everything, jnp.bfloat16),
            dma((phases, n_lon - 1)), dma((phases, n_lon - 1)),
            dma((n_lon // 2 - 1,)), dma((chunks,)),
            dma((chunks, SIDE - 1)), dma((chunks, SIDE - 1)),
            dma, dma((chunks, SIDE, SIDE - 1)),
            dma, dma, dma,
        ],
        compiler_params=pltpu.CompilerParams(
            collective_id=0, has_side_effects=True, dimension_semantics=("arbitrary",)
        ),
    )(transport, sigma_class, basin_id, depth_levels)
    return overturn.reshape(BASINS, HIGH * LOW, -1)[:, :CLASSES]


def solution(mesh):
    placed = (P(None, "lat", "lon"), P(None, "lat", "lon"), P("lat", "lon"), P("lat", "lon"))
    run = functools.partial(body, mesh.shape["lat"], mesh.shape["lon"])
    return jax.shard_map(run, mesh=mesh, in_specs=placed, out_specs=P(), check_vma=False)
```

```python
import functools

import jax
import jax.numpy as jnp
from jax import lax
from jax.experimental import pallas as pl
from jax.experimental.pallas import tpu as pltpu
from jax.sharding import PartitionSpec as P

CLASSES = 200
BASINS = 4
LOW = 32
HIGH = 7
SUB = 8
LANES = 128
SHARE = 4
PHASE = 4
SIDE = 4
MESH = pl.DeviceIdType.MESH


def overturn_kernel(
    n_lat, n_lon, flow_ref, class_ref, basin_ref, depth_ref, out_ref,
    table, parts, shuffle, lines, land,
    sum_send, sum_recv, z_send, z_recv, one_send, one_recv, two_send, two_recv, pair_send, pair_recv, out_sem,
):
    levels, rows, cols = class_ref.shape
    tiles = cols // LANES
    m = BASINS * HIGH * SUB
    n = LOW * SUB
    groups = LANES // SUB
    step = pl.program_id(0)
    steps = pl.num_programs(0)
    phases, owners, size, _ = table.shape
    chunk_rows = phases * size
    chunks = owners // 2
    depth = n_lon // 2
    lat, lon = lax.axis_index("lat"), lax.axis_index("lon")
    x, y = lat // SIDE, lax.rem(lat, SIDE)
    z, core = lon // 2, lax.rem(lon, 2)

    def at(to_lat, to_lon):
        return {"lat": to_lat, "lon": to_lon}

    def along(axis, d):
        if axis == 0:
            return lax.rem(x + d, SIDE) * SIDE + y
        return x * SIDE + lax.rem(y + d, SIDE)

    def block(chunk, of_lat):
        lines_of = pl.ds(pl.multiple_of((2 * chunk + core) * chunk_rows, chunk_rows), chunk_rows)
        return land.at[of_lat, lines_of]

    def send(src, dst, send_sem, recv_sem, to):
        return pltpu.make_async_remote_copy(
            src_ref=src, dst_ref=dst, send_sem=send_sem, recv_sem=recv_sem, device_id=to, device_id_type=MESH
        )

    barrier = pltpu.get_barrier_semaphore()

    @pl.when(step == 0)
    def _():
        for d in range(1, n_lon):
            pl.semaphore_signal(barrier, inc=1, device_id=at(lat, lax.rem(lon + d, n_lon)), device_id_type=MESH)
        for axis in range(2):
            for d in range(1, SIDE):
                pl.semaphore_signal(barrier, inc=1, device_id=at(along(axis, d), lon), device_id_type=MESH)
        line = lax.broadcasted_iota(jnp.int32, (LANES, LANES), 0)
        lane = lax.broadcasted_iota(jnp.int32, (LANES, LANES), 1) & (SUB - 1)
        for low in range(groups):
            at_low = pl.ds(low * LANES, LANES)
            shuffle[:LANES, at_low] = jnp.where(line == lane + low * SUB, 1.0, 0.0).astype(jnp.bfloat16)
            shuffle[LANES:, at_low] = jnp.zeros((LANES, LANES), jnp.bfloat16)
        pl.semaphore_wait(barrier, n_lon - 1 + 2 * (SIDE - 1))


    def twice(v):
        return jnp.concatenate([v, v - 1.0], axis=0).astype(jnp.bfloat16)

    digit = lax.broadcasted_iota(jnp.int32, (2 * LANES, LANES), 1) // (2 * SUB) * 2
    limits = [
        (digit + part * (LANES // SUB)).astype(jnp.float32).astype(jnp.bfloat16) for part in range(n // LANES)
    ]

    def add_products(sub, accs):
        r = pl.ds(sub * SUB, SUB)
        base = [basin_ref[r, pl.ds(tile * LANES, LANES)] * HIGH for tile in range(tiles)]
        wet_levels = [depth_ref[r, pl.ds(tile * LANES, LANES)] for tile in range(tiles)]
        halves = []
        for index in range(levels * tiles):
            k, tile = index // tiles, index % tiles
            c = pl.ds(tile * LANES, LANES)
            klass = class_ref[k, r, c]
            high = jnp.where(k < wet_levels[tile], base[tile] + (klass >> 5), -100)
            low = klass & (LOW - 1)
            flow = flow_ref[k, r, c].astype(jnp.float32)
            halves.append((
                twice(high.astype(jnp.float32)),
                twice(low.astype(jnp.float32)),
                jnp.concatenate([flow, flow], axis=0).astype(jnp.bfloat16),
            ))
            if len(halves) < 2:
                continue
            high2, low2, flow2 = [jnp.concatenate(h, axis=1) for h in zip(*halves)]
            halves = []
            zero = jnp.zeros_like(flow2)
            wide = jnp.concatenate([low2] * (LANES // (2 * SUB)), axis=0).T
            one = jnp.ones_like(wide)
            none = jnp.zeros_like(wide)
            rhs = jnp.concatenate([jnp.where(wide <= limit, one, none) for limit in limits], axis=1)
            lhs = jnp.concatenate(
                [jnp.where(high2 == jnp.bfloat16(2 * t), flow2, zero) for t in range(BASINS * HIGH // 2)], axis=0
            )
            q = (index // 2) % 2
            reg = (index // 4) % 2
            pltpu.matmul_push_rhs(rhs, staging_register=reg, mxu_index=q, transpose=False)
            pltpu.matmul_acc_lhs(accs[q], lhs, load_staged_rhs=reg)

    def finish(group, accs):
        row = lax.broadcasted_iota(jnp.int32, (1, SUB, n), 1)
        col = lax.broadcasted_iota(jnp.int32, (1, SUB, n), 2)
        own = (col & (SUB - 1)) == row
        lane = lax.broadcasted_iota(jnp.int32, (BASINS * HIGH, LANES), 1)
        both = pltpu.matmul_pop(accs[0]) + pltpu.matmul_pop(accs[1])
        part = jnp.sum(jnp.where(own, both.reshape(m // SUB, SUB, n), 0.0), axis=1)
        whole = jnp.where(lane >= LANES - SUB, part[:, n - LANES :], 0.0)
        for shift in (SUB, 2 * SUB, 4 * SUB, 8 * SUB):
            whole = whole + pltpu.roll(whole, shift, 1)
        for basin in range(BASINS):
            before = jnp.zeros((1, LANES), jnp.float32)
            for digit in range(HIGH):
                h = basin * HIGH + digit
                for half in range(n // LANES):
                    owner, share = (2 * h + half) // SHARE, (2 * h + half) % SHARE
                    table[group // PHASE, owner, pl.ds((group & (PHASE - 1)) * SHARE + share, 1), :] = (
                        part[h : h + 1, half * LANES : (half + 1) * LANES] + before
                    )
                before = before + whole[h : h + 1]


    def share_of(phase, d):
        to = lax.rem(lon + d, n_lon)
        return to, send(
            table.at[phase, lax.rem(to, owners)], parts.at[d - 1, phase],
            sum_send.at[phase, d - 1], sum_recv.at[phase, d - 1], at(lat, to),
        )

    def send_phase(phase):
        for d in range(1, n_lon):
            to, copy = share_of(phase, d)

            @pl.when(to < owners)
            def _():
                copy.start()

    def run(even, odd, moved):
        last = steps * 2
        add_products(0, even)
        finish((2 * step + last - 1) & (last - 1), odd)

        @pl.when((step > 0) & ((step & 1) == 0))
        def _():
            send_phase(step // 2 - 1)

        add_products(1, odd)
        finish(2 * step, even)

        @pl.when(step == steps - 1)
        def _():
            finish(last - 1, odd)
            send_phase(phases - 1)
            exchange(moved)


    def exchange(moved):
        partner = at(lat, z * 2 + 1 - core)

        def to_pair(chunk, of_lat):
            send(block(chunk, of_lat), block(chunk, of_lat), pair_send, pair_recv, partner).start()

        @pl.when(lon < owners)
        def _():
            totals = []
            for phase in range(phases):
                total = table[phase, lax.rem(lon, owners)]
                for d in range(1, n_lon):
                    share_of(phase, d)[1].wait_recv()
                    total = total + parts[d - 1, phase]
                totals.append(total)
            total = jnp.concatenate(totals, axis=0).astype(jnp.bfloat16)
            lhs = jnp.concatenate([total, jnp.zeros_like(total)], axis=1)
            row = lax.broadcasted_iota(jnp.int32, (chunk_rows, LANES), 0) // SHARE
            own = row == lax.broadcasted_iota(jnp.int32, (chunk_rows, LANES), 1) // SUB
            for piece in range(groups // 2):
                q = piece % 2
                pltpu.matmul_push_rhs(
                    shuffle[:, pl.ds(piece * 2 * LANES, 2 * LANES)], staging_register=0, mxu_index=q
                )
                pltpu.matmul_acc_lhs(moved[piece], lhs, load_staged_rhs=0)
            for piece in range(groups // 2):
                both = pltpu.matmul_pop(moved[piece])
                for half in range(2):
                    kept = jnp.where(own, both[:, half * LANES : (half + 1) * LANES], 0.0)
                    kept = jnp.sum(kept.reshape(chunk_rows // SUB, SUB, LANES), axis=0)
                    kept = kept[:SHARE] + kept[SHARE:]
                    for share in range(SHARE):
                        at_line = share * groups + piece * 2 + half
                        lines[at_line : at_line + 1, :] = kept[share : share + 1]
            block(z, lat)[...] = lines[...].astype(jnp.bfloat16)
            for d in range(1, depth):
                to = lax.rem(z + d, depth) * 2 + core
                send(block(z, lat), block(z, lat), z_send.at[d - 1], z_recv.at[z], at(lat, to)).start()

        def across(chunk, d_one, d_two):
            swap = lax.rem(chunk, 2)
            dx = d_one + swap * (d_two - d_one)
            dy = d_two + swap * (d_one - d_two)
            return lax.rem(x + dx, SIDE) * SIDE + lax.rem(y + dy, SIDE)

        def first(chunk, d):
            return send(block(chunk, lat), block(chunk, lat), one_send.at[chunk, d - 1], one_recv.at[chunk, d - 1],
                        at(across(chunk, d, 0), lon))

        def second(chunk, of, of_lat, d):
            return send(block(chunk, of_lat), block(chunk, of_lat), two_send, two_recv.at[chunk, of, d - 1],
                        at(across(chunk, 0, d), lon))

        def nearest_first(visit):
            for hop in sorted(range(depth), key=lambda hop: min(hop, depth - hop)):
                chunk = lax.rem(z + hop, depth)
                pl.when(chunk < chunks)(functools.partial(visit, chunk, hop))

        def arrive(chunk, hop):
            if hop:
                send(block(chunk, lat), block(chunk, lat), z_send.at[0], z_recv.at[chunk], at(lat, lon)).wait_recv()
            for d in range(1, SIDE):
                first(chunk, d).start()
            for d in range(1, SIDE):
                second(chunk, 0, lat, d).start()
            to_pair(chunk, lat)

        def turn(chunk, hop):
            for of in range(1, SIDE):
                first(chunk, of).wait_recv()
                came = across(chunk, SIDE - of, 0)
                for d in range(1, SIDE):
                    second(chunk, of, came, d).start()
                to_pair(chunk, came)

        def settle(chunk, hop):
            for of in range(SIDE):
                for d in range(1, SIDE):
                    second(chunk, of, lat, d).wait_recv()
                    to_pair(chunk, across(chunk, SIDE - of, SIDE - d))

        nearest_first(arrive)
        nearest_first(turn)
        nearest_first(settle)

        half = land.at[pl.ds(0, n_lat // 2)]
        pltpu.make_async_copy(half, half, pair_recv).wait()
        outs = [
            pltpu.make_async_copy(land.at[of], out_ref.at[:, pl.ds(of * LANES, LANES)], out_sem.at[of])
            for of in range(n_lat)
        ]
        for out in outs:
            out.start()
        for phase in range(phases):
            for d in range(1, n_lon):
                to, copy = share_of(phase, d)

                @pl.when(to < owners)
                def _():
                    copy.wait_send()

        @pl.when(lon < owners)
        def _():
            for d in range(1, depth):
                send(block(z, lat), block(z, lat), z_send.at[d - 1], z_recv.at[z], at(lat, lon)).wait_send()

        for chunk in range(chunks):
            for d in range(1, SIDE):
                first(chunk, d).wait_send()
        seconds = land.at[pl.ds(0, chunks * SIDE * (SIDE - 1) * chunk_rows // land.shape[1])]
        pltpu.make_async_copy(seconds, seconds, two_send).wait()
        pltpu.make_async_copy(half, half, pair_send).wait()
        for out in outs:
            out.wait()

    def acc(q, lines_of):
        return pltpu.ACC(q)((lines_of, n), jnp.float32)

    pl.run_scoped(
        run,
        tuple(acc(q, m) for q in range(2)),
        tuple(acc(q, m) for q in range(2)),
        tuple(acc(piece % 2, chunk_rows) for piece in range(groups // 2)),
    )


def keep_kernel(all_ref, kept_ref, held, in_sem, out_sem):
    ins = [
        pltpu.make_async_copy(all_ref.at[b, pl.ds(0, CLASSES)], held.at[b], in_sem.at[b]) for b in range(BASINS)
    ]
    outs = [pltpu.make_async_copy(held.at[b], kept_ref.at[b], out_sem.at[b]) for b in range(BASINS)]
    for copy in ins:
        copy.start()
    for b in range(BASINS):
        ins[b].wait()
        outs[b].start()
    for copy in outs:
        copy.wait()


def body(n_lat, n_lon, transport, sigma_class, basin_id, depth_levels):
    levels, rows, cols = sigma_class.shape
    step_rows = 2 * SUB
    owners = BASINS * HIGH * LOW * SUB // LANES // SHARE
    chunks = owners // 2
    phases = rows // SUB // PHASE
    size = SHARE * PHASE
    dma = pltpu.SemaphoreType.DMA
    everything = (owners * phases * size, n_lat * LANES)
    overturn = pl.pallas_call(
        functools.partial(overturn_kernel, n_lat, n_lon),
        grid=(rows // step_rows,),
        in_specs=[
            pl.BlockSpec((levels, step_rows, cols), lambda g: (0, g, 0)),
            pl.BlockSpec((levels, step_rows, cols), lambda g: (0, g, 0)),
            pl.BlockSpec((step_rows, cols), lambda g: (g, 0)),
            pl.BlockSpec((step_rows, cols), lambda g: (g, 0)),
        ],
        out_specs=pl.BlockSpec(memory_space=pl.ANY),
        out_shape=jax.ShapeDtypeStruct(everything, jnp.bfloat16),
        scratch_shapes=[
            pltpu.VMEM((phases, owners, size, LANES), jnp.float32),
            pltpu.VMEM((n_lon - 1, phases, size, LANES), jnp.float32),
            pltpu.VMEM((2 * LANES, LANES // SUB * LANES), jnp.bfloat16),
            pltpu.VMEM((phases * size, LANES), jnp.float32),
            pltpu.VMEM((n_lat, everything[0], LANES), jnp.bfloat16),
            dma((phases, n_lon - 1)), dma((phases, n_lon - 1)),
            dma((n_lon // 2 - 1,)), dma((chunks,)),
            dma((chunks, SIDE - 1)), dma((chunks, SIDE - 1)),
            dma, dma((chunks, SIDE, SIDE - 1)),
            dma, dma, dma((n_lat,)),
        ],
        compiler_params=pltpu.CompilerParams(
            collective_id=0, has_side_effects=True, dimension_semantics=("arbitrary",)
        ),
    )(transport, sigma_class, basin_id, depth_levels)
    kept = jax.ShapeDtypeStruct((BASINS, CLASSES, n_lat * LANES), jnp.bfloat16)
    return pl.pallas_call(
        keep_kernel,
        out_shape=kept,
        in_specs=[pl.BlockSpec(memory_space=pl.ANY)],
        out_specs=pl.BlockSpec(memory_space=pl.ANY),
        scratch_shapes=[pltpu.VMEM(kept.shape, kept.dtype), dma((BASINS,)), dma((BASINS,))],
    )(overturn.reshape(BASINS, HIGH * LOW, -1))


def solution(mesh):
    placed = (P(None, "lat", "lon"), P(None, "lat", "lon"), P("lat", "lon"), P("lat", "lon"))
    run = functools.partial(body, mesh.shape["lat"], mesh.shape["lon"])
    return jax.shard_map(run, mesh=mesh, in_specs=placed, out_specs=P(), check_vma=False)
```

```python
import functools

import jax
import jax.numpy as jnp
from jax import lax
from jax.experimental import pallas as pl
from jax.experimental.pallas import tpu as pltpu
from jax.sharding import PartitionSpec as P

CLASSES = 200
BASINS = 4
LOW = 32
HIGH = 7
SUB = 8
LANES = 128
SHARE = 4
PHASE = 2
SIDE = 4
MESH = pl.DeviceIdType.MESH


def overturn_kernel(
    n_lat, n_lon, flow_ref, class_ref, basin_ref, depth_ref, out_ref,
    table, parts, shuffle, lines, land,
    sum_send, sum_recv, z_send, z_recv, one_send, one_recv, two_send, two_recv, pair_send, pair_recv, out_sem,
):
    levels, rows, cols = class_ref.shape
    tiles = cols // LANES
    m = BASINS * HIGH * SUB
    n = LOW * SUB
    groups = LANES // SUB
    step = pl.program_id(0)
    steps = pl.num_programs(0)
    phases, owners, size, _ = table.shape
    chunk_rows = phases * size
    chunks = owners // 2
    depth = n_lon // 2
    lat, lon = lax.axis_index("lat"), lax.axis_index("lon")
    x, y = lat // SIDE, lax.rem(lat, SIDE)
    z, core = lon // 2, lax.rem(lon, 2)

    def at(to_lat, to_lon):
        return {"lat": to_lat, "lon": to_lon}

    def along(axis, d):
        if axis == 0:
            return lax.rem(x + d, SIDE) * SIDE + y
        return x * SIDE + lax.rem(y + d, SIDE)

    def block(chunk, of_lat):
        lines_of = pl.ds(pl.multiple_of((2 * chunk + core) * chunk_rows, chunk_rows), chunk_rows)
        return land.at[of_lat, lines_of]

    def send(src, dst, send_sem, recv_sem, to):
        return pltpu.make_async_remote_copy(
            src_ref=src, dst_ref=dst, send_sem=send_sem, recv_sem=recv_sem, device_id=to, device_id_type=MESH
        )

    barrier = pltpu.get_barrier_semaphore()

    @pl.when(step == 0)
    def _():
        for d in range(1, n_lon):
            pl.semaphore_signal(barrier, inc=1, device_id=at(lat, lax.rem(lon + d, n_lon)), device_id_type=MESH)
        for axis in range(2):
            for d in range(1, SIDE):
                pl.semaphore_signal(barrier, inc=1, device_id=at(along(axis, d), lon), device_id_type=MESH)
        line = lax.broadcasted_iota(jnp.int32, (LANES, LANES), 0)
        lane = lax.broadcasted_iota(jnp.int32, (LANES, LANES), 1) & (SUB - 1)
        for low in range(groups):
            at_low = pl.ds(low * LANES, LANES)
            shuffle[:LANES, at_low] = jnp.where(line == lane + low * SUB, 1.0, 0.0).astype(jnp.bfloat16)
            shuffle[LANES:, at_low] = jnp.zeros((LANES, LANES), jnp.bfloat16)


    def twice(v):
        return jnp.concatenate([v, v - 1.0], axis=0).astype(jnp.bfloat16)

    digit = lax.broadcasted_iota(jnp.int32, (2 * LANES, LANES), 1) // (2 * SUB) * 2
    limits = [
        (digit + part * (LANES // SUB)).astype(jnp.float32).astype(jnp.bfloat16) for part in range(n // LANES)
    ]

    def add_products(sub, accs):
        r = pl.ds(sub * SUB, SUB)
        base = [basin_ref[r, pl.ds(tile * LANES, LANES)] * HIGH for tile in range(tiles)]
        wet_levels = [depth_ref[r, pl.ds(tile * LANES, LANES)] for tile in range(tiles)]
        halves = []
        for index in range(levels * tiles):
            k, tile = index // tiles, index % tiles
            c = pl.ds(tile * LANES, LANES)
            klass = class_ref[k, r, c]
            high = jnp.where(k < wet_levels[tile], base[tile] + (klass >> 5), -100)
            low = klass & (LOW - 1)
            flow = flow_ref[k, r, c].astype(jnp.float32)
            halves.append((
                twice(high.astype(jnp.float32)),
                twice(low.astype(jnp.float32)),
                jnp.concatenate([flow, flow], axis=0).astype(jnp.bfloat16),
            ))
            if len(halves) < 2:
                continue
            high2, low2, flow2 = [jnp.concatenate(h, axis=1) for h in zip(*halves)]
            halves = []
            zero = jnp.zeros_like(flow2)
            wide = jnp.concatenate([low2] * (LANES // (2 * SUB)), axis=0).T
            one = jnp.ones_like(wide)
            none = jnp.zeros_like(wide)
            rhs = jnp.concatenate([jnp.where(wide <= limit, one, none) for limit in limits], axis=1)
            lhs = jnp.concatenate(
                [jnp.where(high2 == jnp.bfloat16(2 * t), flow2, zero) for t in range(BASINS * HIGH // 2)], axis=0
            )
            q = (index // 2) % 2
            reg = (index // 4) % 2
            pltpu.matmul_push_rhs(rhs, staging_register=reg, mxu_index=q, transpose=False)
            pltpu.matmul_acc_lhs(accs[q], lhs, load_staged_rhs=reg)

    def finish(group, accs):
        row = lax.broadcasted_iota(jnp.int32, (1, SUB, n), 1)
        col = lax.broadcasted_iota(jnp.int32, (1, SUB, n), 2)
        own = (col & (SUB - 1)) == row
        lane = lax.broadcasted_iota(jnp.int32, (BASINS * HIGH, LANES), 1)
        both = pltpu.matmul_pop(accs[0]) + pltpu.matmul_pop(accs[1])
        part = jnp.sum(jnp.where(own, both.reshape(m // SUB, SUB, n), 0.0), axis=1)
        whole = jnp.where(lane >= LANES - SUB, part[:, n - LANES :], 0.0)
        for shift in (SUB, 2 * SUB, 4 * SUB, 8 * SUB):
            whole = whole + pltpu.roll(whole, shift, 1)
        for basin in range(BASINS):
            before = jnp.zeros((1, LANES), jnp.float32)
            for digit in range(HIGH):
                h = basin * HIGH + digit
                for half in range(n // LANES):
                    owner, share = (2 * h + half) // SHARE, (2 * h + half) % SHARE
                    table[group // PHASE, owner, pl.ds((group & (PHASE - 1)) * SHARE + share, 1), :] = (
                        part[h : h + 1, half * LANES : (half + 1) * LANES] + before
                    )
                before = before + whole[h : h + 1]


    def share_of(phase, d):
        to = lax.rem(lon + d, n_lon)
        return to, send(
            table.at[phase, lax.rem(to, owners)], parts.at[d - 1, phase],
            sum_send.at[phase, d - 1], sum_recv.at[phase, d - 1], at(lat, to),
        )

    def send_phase(phase):
        for d in range(1, n_lon):
            to, copy = share_of(phase, d)

            @pl.when(to < owners)
            def _():
                copy.start()

    def run(even, odd, moved):
        last = steps * 2
        add_products(0, even)
        finish((2 * step + last - 1) & (last - 1), odd)

        @pl.when(step == 2)
        def _():
            pl.semaphore_wait(barrier, n_lon - 1 + 2 * (SIDE - 1))

        @pl.when((step > 0) & ((step & 1) == 0))
        def _():
            send_phase(step - 2)
            send_phase(step - 1)

        @pl.when(step == steps - 1)
        def _():
            send_phase(phases - 2)

        add_products(1, odd)
        finish(2 * step, even)

        @pl.when(step == steps - 1)
        def _():
            finish(last - 1, odd)
            send_phase(phases - 1)
            exchange(moved)


    def exchange(moved):
        partner = at(lat, z * 2 + 1 - core)

        def to_pair(chunk, of_lat):
            send(block(chunk, of_lat), block(chunk, of_lat), pair_send, pair_recv, partner).start()

        @pl.when(lon < owners)
        def _():
            totals = []
            for phase in range(phases):
                total = table[phase, lax.rem(lon, owners)]
                for d in range(1, n_lon):
                    share_of(phase, d)[1].wait_recv()
                    total = total + parts[d - 1, phase]
                totals.append(total)
            total = jnp.concatenate(totals, axis=0).astype(jnp.bfloat16)
            lhs = jnp.concatenate([total, jnp.zeros_like(total)], axis=1)
            row = lax.broadcasted_iota(jnp.int32, (chunk_rows, LANES), 0) // SHARE
            own = row == lax.broadcasted_iota(jnp.int32, (chunk_rows, LANES), 1) // SUB
            for piece in range(groups // 2):
                q = piece % 2
                pltpu.matmul_push_rhs(
                    shuffle[:, pl.ds(piece * 2 * LANES, 2 * LANES)], staging_register=0, mxu_index=q
                )
                pltpu.matmul_acc_lhs(moved[piece], lhs, load_staged_rhs=0)
            for piece in range(groups // 2):
                both = pltpu.matmul_pop(moved[piece])
                for half in range(2):
                    kept = jnp.where(own, both[:, half * LANES : (half + 1) * LANES], 0.0)
                    kept = jnp.sum(kept.reshape(chunk_rows // SUB, SUB, LANES), axis=0)
                    kept = kept[:SHARE] + kept[SHARE:]
                    for share in range(SHARE):
                        at_line = share * groups + piece * 2 + half
                        lines[at_line : at_line + 1, :] = kept[share : share + 1]
            block(z, lat)[...] = lines[...].astype(jnp.bfloat16)
            for d in range(1, depth):
                to = lax.rem(z + d, depth) * 2 + core
                send(block(z, lat), block(z, lat), z_send.at[d - 1], z_recv.at[z], at(lat, to)).start()

        def across(chunk, d_one, d_two):
            swap = lax.rem(chunk + core, 2)
            dx = d_one + swap * (d_two - d_one)
            dy = d_two + swap * (d_one - d_two)
            return lax.rem(x + dx, SIDE) * SIDE + lax.rem(y + dy, SIDE)

        def first(chunk, d):
            return send(block(chunk, lat), block(chunk, lat), one_send.at[chunk, d - 1], one_recv.at[chunk, d - 1],
                        at(across(chunk, d, 0), lon))

        def second(chunk, of, of_lat, d):
            return send(block(chunk, of_lat), block(chunk, of_lat), two_send, two_recv.at[chunk, of, d - 1],
                        at(across(chunk, 0, d), lon))

        def nearest_first(visit):
            for hop in sorted(range(depth), key=lambda hop: min(hop, depth - hop)):
                chunk = lax.rem(z + hop, depth)
                pl.when(chunk < chunks)(functools.partial(visit, chunk, hop))

        def arrive(chunk, hop):
            if hop:
                send(block(chunk, lat), block(chunk, lat), z_send.at[0], z_recv.at[chunk], at(lat, lon)).wait_recv()
            for d in range(1, SIDE):
                first(chunk, d).start()
            for d in range(1, SIDE):
                second(chunk, 0, lat, d).start()
            to_pair(chunk, lat)

        def turn(chunk, hop):
            for of in range(1, SIDE):
                first(chunk, of).wait_recv()
                came = across(chunk, SIDE - of, 0)
                for d in range(1, SIDE):
                    second(chunk, of, came, d).start()
                to_pair(chunk, came)

        def settle(chunk, hop):
            for of in range(SIDE):
                for d in range(1, SIDE):
                    second(chunk, of, lat, d).wait_recv()
                    to_pair(chunk, across(chunk, SIDE - of, SIDE - d))

        nearest_first(arrive)
        nearest_first(turn)
        nearest_first(settle)

        half = land.at[pl.ds(0, n_lat // 2)]
        pltpu.make_async_copy(half, half, pair_recv).wait()
        outs = [
            pltpu.make_async_copy(land.at[of], out_ref.at[:, pl.ds(of * LANES, LANES)], out_sem.at[of])
            for of in range(n_lat)
        ]
        for out in outs:
            out.start()
        for phase in range(phases):
            for d in range(1, n_lon):
                to, copy = share_of(phase, d)

                @pl.when(to < owners)
                def _():
                    copy.wait_send()

        @pl.when(lon < owners)
        def _():
            for d in range(1, depth):
                send(block(z, lat), block(z, lat), z_send.at[d - 1], z_recv.at[z], at(lat, lon)).wait_send()

        for chunk in range(chunks):
            for d in range(1, SIDE):
                first(chunk, d).wait_send()
        seconds = land.at[pl.ds(0, chunks * SIDE * (SIDE - 1) * chunk_rows // land.shape[1])]
        pltpu.make_async_copy(seconds, seconds, two_send).wait()
        pltpu.make_async_copy(half, half, pair_send).wait()
        for out in outs:
            out.wait()

    def acc(q, lines_of):
        return pltpu.ACC(q)((lines_of, n), jnp.float32)

    pl.run_scoped(
        run,
        tuple(acc(q, m) for q in range(2)),
        tuple(acc(q, m) for q in range(2)),
        tuple(acc(piece % 2, chunk_rows) for piece in range(groups // 2)),
    )


def keep_kernel(all_ref, kept_ref, held, in_sem, out_sem):
    ins = [
        pltpu.make_async_copy(all_ref.at[b, pl.ds(0, CLASSES)], held.at[b], in_sem.at[b]) for b in range(BASINS)
    ]
    outs = [pltpu.make_async_copy(held.at[b], kept_ref.at[b], out_sem.at[b]) for b in range(BASINS)]
    for copy in ins:
        copy.start()
    for b in range(BASINS):
        ins[b].wait()
        outs[b].start()
    for copy in outs:
        copy.wait()


def body(n_lat, n_lon, transport, sigma_class, basin_id, depth_levels):
    levels, rows, cols = sigma_class.shape
    step_rows = 2 * SUB
    owners = BASINS * HIGH * LOW * SUB // LANES // SHARE
    chunks = owners // 2
    phases = rows // SUB // PHASE
    size = SHARE * PHASE
    dma = pltpu.SemaphoreType.DMA
    everything = (owners * phases * size, n_lat * LANES)
    overturn = pl.pallas_call(
        functools.partial(overturn_kernel, n_lat, n_lon),
        grid=(rows // step_rows,),
        in_specs=[
            pl.BlockSpec((levels, step_rows, cols), lambda g: (0, g, 0)),
            pl.BlockSpec((levels, step_rows, cols), lambda g: (0, g, 0)),
            pl.BlockSpec((step_rows, cols), lambda g: (g, 0)),
            pl.BlockSpec((step_rows, cols), lambda g: (g, 0)),
        ],
        out_specs=pl.BlockSpec(memory_space=pl.ANY),
        out_shape=jax.ShapeDtypeStruct(everything, jnp.bfloat16),
        scratch_shapes=[
            pltpu.VMEM((phases, owners, size, LANES), jnp.float32),
            pltpu.VMEM((n_lon - 1, phases, size, LANES), jnp.float32),
            pltpu.VMEM((2 * LANES, LANES // SUB * LANES), jnp.bfloat16),
            pltpu.VMEM((phases * size, LANES), jnp.float32),
            pltpu.VMEM((n_lat, everything[0], LANES), jnp.bfloat16),
            dma((phases, n_lon - 1)), dma((phases, n_lon - 1)),
            dma((n_lon // 2 - 1,)), dma((chunks,)),
            dma((chunks, SIDE - 1)), dma((chunks, SIDE - 1)),
            dma, dma((chunks, SIDE, SIDE - 1)),
            dma, dma, dma((n_lat,)),
        ],
        compiler_params=pltpu.CompilerParams(
            collective_id=0, has_side_effects=True, dimension_semantics=("arbitrary",)
        ),
    )(transport, sigma_class, basin_id, depth_levels)
    kept = jax.ShapeDtypeStruct((BASINS, CLASSES, n_lat * LANES), jnp.bfloat16)
    return pl.pallas_call(
        keep_kernel,
        out_shape=kept,
        in_specs=[pl.BlockSpec(memory_space=pl.ANY)],
        out_specs=pl.BlockSpec(memory_space=pl.ANY),
        scratch_shapes=[pltpu.VMEM(kept.shape, kept.dtype), dma((BASINS,)), dma((BASINS,))],
    )(overturn.reshape(BASINS, HIGH * LOW, -1))


def solution(mesh):
    placed = (P(None, "lat", "lon"), P(None, "lat", "lon"), P("lat", "lon"), P("lat", "lon"))
    run = functools.partial(body, mesh.shape["lat"], mesh.shape["lon"])
    return jax.shard_map(run, mesh=mesh, in_specs=placed, out_specs=P(), check_vma=False)
```

```python
import functools

import jax
import jax.numpy as jnp
from jax import lax
from jax.experimental import pallas as pl
from jax.experimental.pallas import tpu as pltpu
from jax.sharding import PartitionSpec as P

CLASSES = 200
BASINS = 4
LOW = 32
HIGH = 7
SUB = 8
LANES = 128
SHARE = 4
PHASE = 2
SIDE = 4
MESH = pl.DeviceIdType.MESH


def overturn_kernel(
    n_lat, n_lon, flow_ref, class_ref, basin_ref, depth_ref, out_ref,
    table, parts, shuffle, lines, land,
    sum_send, sum_recv, z_send, z_recv, one_send, one_recv, two_send, two_recv, pair_send, pair_recv, out_sem,
):
    levels, rows, cols = class_ref.shape
    tiles = cols // LANES
    m = BASINS * HIGH * SUB
    n = LOW * SUB
    groups = LANES // SUB
    step = pl.program_id(0)
    steps = pl.num_programs(0)
    phases, owners, size, _ = table.shape
    chunk_rows = phases * size
    chunks = owners // 2
    depth = n_lon // 2
    lat, lon = lax.axis_index("lat"), lax.axis_index("lon")
    x, y = lat // SIDE, lax.rem(lat, SIDE)
    z, core = lon // 2, lax.rem(lon, 2)

    def at(to_lat, to_lon):
        return {"lat": to_lat, "lon": to_lon}

    def along(axis, d):
        if axis == 0:
            return lax.rem(x + d, SIDE) * SIDE + y
        return x * SIDE + lax.rem(y + d, SIDE)

    def block(chunk, of_lat):
        lines_of = pl.ds(pl.multiple_of((2 * chunk + core) * chunk_rows, chunk_rows), chunk_rows)
        return land.at[of_lat, lines_of]

    def send(src, dst, send_sem, recv_sem, to):
        return pltpu.make_async_remote_copy(
            src_ref=src, dst_ref=dst, send_sem=send_sem, recv_sem=recv_sem, device_id=to, device_id_type=MESH
        )

    barrier = pltpu.get_barrier_semaphore()

    @pl.when(step == 0)
    def _():
        for d in range(1, n_lon):
            pl.semaphore_signal(barrier, inc=1, device_id=at(lat, lax.rem(lon + d, n_lon)), device_id_type=MESH)
        for axis in range(2):
            for d in range(1, SIDE):
                pl.semaphore_signal(barrier, inc=1, device_id=at(along(axis, d), lon), device_id_type=MESH)
        line = lax.broadcasted_iota(jnp.int32, (LANES, LANES), 0)
        lane = lax.broadcasted_iota(jnp.int32, (LANES, LANES), 1) & (SUB - 1)
        for low in range(groups):
            at_low = pl.ds(low * LANES, LANES)
            shuffle[:LANES, at_low] = jnp.where(line == lane + low * SUB, 1.0, 0.0).astype(jnp.bfloat16)
            shuffle[LANES:, at_low] = jnp.zeros((LANES, LANES), jnp.bfloat16)


    def twice(v):
        return jnp.concatenate([v, v - 1.0], axis=0).astype(jnp.bfloat16)

    digit = lax.broadcasted_iota(jnp.int32, (2 * LANES, LANES), 1) // (2 * SUB) * 2
    limits = [
        (digit + part * (LANES // SUB)).astype(jnp.float32).astype(jnp.bfloat16) for part in range(n // LANES)
    ]

    def add_products(sub, accs):
        r = pl.ds(sub * SUB, SUB)
        base = [basin_ref[r, pl.ds(tile * LANES, LANES)] * HIGH for tile in range(tiles)]
        wet_levels = [depth_ref[r, pl.ds(tile * LANES, LANES)] for tile in range(tiles)]
        halves = []
        for index in range(levels * tiles):
            k, tile = index // tiles, index % tiles
            c = pl.ds(tile * LANES, LANES)
            klass = class_ref[k, r, c]
            high = jnp.where(k < wet_levels[tile], base[tile] + (klass >> 5), -100)
            low = klass & (LOW - 1)
            flow = flow_ref[k, r, c].astype(jnp.float32)
            halves.append((
                twice(high.astype(jnp.float32)),
                twice(low.astype(jnp.float32)),
                jnp.concatenate([flow, flow], axis=0).astype(jnp.bfloat16),
            ))
            if len(halves) < 2:
                continue
            high2, low2, flow2 = [jnp.concatenate(h, axis=1) for h in zip(*halves)]
            halves = []
            zero = jnp.zeros_like(flow2)
            wide = jnp.concatenate([low2] * (LANES // (2 * SUB)), axis=0).T
            one = jnp.ones_like(wide)
            none = jnp.zeros_like(wide)
            rhs = jnp.concatenate([jnp.where(wide <= limit, one, none) for limit in limits], axis=1)
            lhs = jnp.concatenate(
                [jnp.where(high2 == jnp.bfloat16(2 * t), flow2, zero) for t in range(BASINS * HIGH // 2)], axis=0
            )
            q = (index // 2) % 2
            reg = (index // 4) % 2
            pltpu.matmul_push_rhs(rhs, staging_register=reg, mxu_index=q, transpose=False)
            pltpu.matmul_acc_lhs(accs[q], lhs, load_staged_rhs=reg)

    def finish(group, accs):
        row = lax.broadcasted_iota(jnp.int32, (1, SUB, n), 1)
        col = lax.broadcasted_iota(jnp.int32, (1, SUB, n), 2)
        own = (col & (SUB - 1)) == row
        lane = lax.broadcasted_iota(jnp.int32, (BASINS * HIGH, LANES), 1)
        both = pltpu.matmul_pop(accs[0]) + pltpu.matmul_pop(accs[1])
        part = jnp.sum(jnp.where(own, both.reshape(m // SUB, SUB, n), 0.0), axis=1)
        whole = jnp.where(lane >= LANES - SUB, part[:, n - LANES :], 0.0)
        for shift in (SUB, 2 * SUB, 4 * SUB, 8 * SUB):
            whole = whole + pltpu.roll(whole, shift, 1)
        for basin in range(BASINS):
            before = jnp.zeros((1, LANES), jnp.float32)
            for digit in range(HIGH):
                h = basin * HIGH + digit
                for half in range(n // LANES):
                    owner, share = (2 * h + half) // SHARE, (2 * h + half) % SHARE
                    table[group // PHASE, owner, pl.ds((group & (PHASE - 1)) * SHARE + share, 1), :] = (
                        part[h : h + 1, half * LANES : (half + 1) * LANES] + before
                    )
                before = before + whole[h : h + 1]


    def share_of(phase, d):
        to = lax.rem(lon + d, n_lon)
        return to, send(
            table.at[phase, lax.rem(to, owners)], parts.at[d - 1, phase],
            sum_send.at[phase, d - 1], sum_recv.at[phase, d - 1], at(lat, to),
        )

    def send_phase(phase):
        for d in range(1, n_lon):
            to, copy = share_of(phase, d)

            @pl.when(to < owners)
            def _():
                copy.start()

    def run(even, odd, moved):
        last = steps * 2
        add_products(0, even)
        finish((2 * step + last - 1) & (last - 1), odd)

        @pl.when(step == 2)
        def _():
            pl.semaphore_wait(barrier, n_lon - 1 + 2 * (SIDE - 1))

        @pl.when((step > 0) & ((step & 1) == 0))
        def _():
            send_phase(step - 2)
            send_phase(step - 1)

        @pl.when(step == steps - 1)
        def _():
            send_phase(phases - 2)

        add_products(1, odd)
        finish(2 * step, even)

        @pl.when(step == steps - 1)
        def _():
            finish(last - 1, odd)
            send_phase(phases - 1)
            exchange(moved)


    def exchange(moved):
        partner = at(lat, z * 2 + 1 - core)

        def shares_left(phase):
            for d in range(1, n_lon):
                to, copy = share_of(phase, d)

                @pl.when(to < owners)
                def _():
                    copy.wait_send()

        for phase in range(phases - 1):
            shares_left(phase)

        def to_pair(chunk, of_lat):
            send(block(chunk, of_lat), block(chunk, of_lat), pair_send, pair_recv, partner).start()

        @pl.when(lon < owners)
        def _():
            totals = []
            for phase in range(phases):
                total = table[phase, lax.rem(lon, owners)]
                for d in range(1, n_lon):
                    share_of(phase, d)[1].wait_recv()
                    total = total + parts[d - 1, phase]
                totals.append(total)
            total = jnp.concatenate(totals, axis=0).astype(jnp.bfloat16)
            lhs = jnp.concatenate([total, jnp.zeros_like(total)], axis=1)
            row = lax.broadcasted_iota(jnp.int32, (chunk_rows, LANES), 0) // SHARE
            own = row == lax.broadcasted_iota(jnp.int32, (chunk_rows, LANES), 1) // SUB
            for piece in range(groups // 2):
                q = piece % 2
                pltpu.matmul_push_rhs(
                    shuffle[:, pl.ds(piece * 2 * LANES, 2 * LANES)], staging_register=0, mxu_index=q
                )
                pltpu.matmul_acc_lhs(moved[piece], lhs, load_staged_rhs=0)
            for piece in range(groups // 2):
                both = pltpu.matmul_pop(moved[piece])
                for half in range(2):
                    kept = jnp.where(own, both[:, half * LANES : (half + 1) * LANES], 0.0)
                    kept = jnp.sum(kept.reshape(chunk_rows // SUB, SUB, LANES), axis=0)
                    kept = kept[:SHARE] + kept[SHARE:]
                    for share in range(SHARE):
                        at_line = share * groups + piece * 2 + half
                        lines[at_line : at_line + 1, :] = kept[share : share + 1]
            block(z, lat)[...] = lines[...].astype(jnp.bfloat16)
            for d in sorted(range(1, depth), key=lambda d: min(d, depth - d)):
                to = lax.rem(z + d, depth) * 2 + core
                send(block(z, lat), block(z, lat), z_send.at[d - 1], z_recv.at[z], at(lat, to)).start()

        def across(chunk, d_one, d_two):
            swap = lax.rem(chunk + core, 2)
            dx = d_one + swap * (d_two - d_one)
            dy = d_two + swap * (d_one - d_two)
            return lax.rem(x + dx, SIDE) * SIDE + lax.rem(y + dy, SIDE)

        def first(chunk, d):
            return send(block(chunk, lat), block(chunk, lat), one_send.at[chunk, d - 1], one_recv.at[chunk, d - 1],
                        at(across(chunk, d, 0), lon))

        def second(chunk, of, of_lat, d):
            return send(block(chunk, of_lat), block(chunk, of_lat), two_send, two_recv.at[chunk, of, d - 1],
                        at(across(chunk, 0, d), lon))

        def nearest_first(visit):
            for hop in sorted(range(depth), key=lambda hop: min(hop, depth - hop)):
                chunk = lax.rem(z + hop, depth)
                pl.when(chunk < chunks)(functools.partial(visit, chunk, hop))

        def arrive(chunk, hop):
            if hop:
                send(block(chunk, lat), block(chunk, lat), z_send.at[0], z_recv.at[chunk], at(lat, lon)).wait_recv()
            for d in range(1, SIDE):
                first(chunk, d).start()
            for d in range(1, SIDE):
                second(chunk, 0, lat, d).start()
            to_pair(chunk, lat)

        def turn(chunk, hop):
            for of in range(1, SIDE):
                first(chunk, of).wait_recv()
                came = across(chunk, SIDE - of, 0)
                for d in range(1, SIDE):
                    second(chunk, of, came, d).start()
                to_pair(chunk, came)

        def settle(chunk, hop):
            for of in range(SIDE):
                for d in range(1, SIDE):
                    second(chunk, of, lat, d).wait_recv()
                    to_pair(chunk, across(chunk, SIDE - of, SIDE - d))

        shares_left(phases - 1)
        nearest_first(arrive)
        nearest_first(turn)

        @pl.when(lon < owners)
        def _():
            for d in range(1, depth):
                send(block(z, lat), block(z, lat), z_send.at[d - 1], z_recv.at[z], at(lat, lon)).wait_send()

        for chunk in range(chunks):
            for d in range(1, SIDE):
                first(chunk, d).wait_send()
        nearest_first(settle)

        half = land.at[pl.ds(0, n_lat // 2)]
        pltpu.make_async_copy(half, half, pair_recv).wait()
        outs = [
            pltpu.make_async_copy(land.at[of], out_ref.at[:, pl.ds(of * LANES, LANES)], out_sem.at[of])
            for of in range(n_lat)
        ]
        for out in outs:
            out.start()
        seconds = land.at[pl.ds(0, chunks * SIDE * (SIDE - 1) * chunk_rows // land.shape[1])]
        pltpu.make_async_copy(seconds, seconds, two_send).wait()
        pltpu.make_async_copy(half, half, pair_send).wait()
        for out in outs:
            out.wait()

    def acc(q, lines_of):
        return pltpu.ACC(q)((lines_of, n), jnp.float32)

    pl.run_scoped(
        run,
        tuple(acc(q, m) for q in range(2)),
        tuple(acc(q, m) for q in range(2)),
        tuple(acc(piece % 2, chunk_rows) for piece in range(groups // 2)),
    )


def keep_kernel(all_ref, kept_ref, held, in_sem, out_sem):
    ins = [
        pltpu.make_async_copy(all_ref.at[b, pl.ds(0, CLASSES)], held.at[b], in_sem.at[b]) for b in range(BASINS)
    ]
    outs = [pltpu.make_async_copy(held.at[b], kept_ref.at[b], out_sem.at[b]) for b in range(BASINS)]
    for copy in ins:
        copy.start()
    for b in range(BASINS):
        ins[b].wait()
        outs[b].start()
    for copy in outs:
        copy.wait()


def body(n_lat, n_lon, transport, sigma_class, basin_id, depth_levels):
    levels, rows, cols = sigma_class.shape
    step_rows = 2 * SUB
    owners = BASINS * HIGH * LOW * SUB // LANES // SHARE
    chunks = owners // 2
    phases = rows // SUB // PHASE
    size = SHARE * PHASE
    dma = pltpu.SemaphoreType.DMA
    everything = (owners * phases * size, n_lat * LANES)
    overturn = pl.pallas_call(
        functools.partial(overturn_kernel, n_lat, n_lon),
        grid=(rows // step_rows,),
        in_specs=[
            pl.BlockSpec((levels, step_rows, cols), lambda g: (0, g, 0)),
            pl.BlockSpec((levels, step_rows, cols), lambda g: (0, g, 0)),
            pl.BlockSpec((step_rows, cols), lambda g: (g, 0)),
            pl.BlockSpec((step_rows, cols), lambda g: (g, 0)),
        ],
        out_specs=pl.BlockSpec(memory_space=pl.ANY),
        out_shape=jax.ShapeDtypeStruct(everything, jnp.bfloat16),
        scratch_shapes=[
            pltpu.VMEM((phases, owners, size, LANES), jnp.float32),
            pltpu.VMEM((n_lon - 1, phases, size, LANES), jnp.float32),
            pltpu.VMEM((2 * LANES, LANES // SUB * LANES), jnp.bfloat16),
            pltpu.VMEM((phases * size, LANES), jnp.float32),
            pltpu.VMEM((n_lat, everything[0], LANES), jnp.bfloat16),
            dma((phases, n_lon - 1)), dma((phases, n_lon - 1)),
            dma((n_lon // 2 - 1,)), dma((chunks,)),
            dma((chunks, SIDE - 1)), dma((chunks, SIDE - 1)),
            dma, dma((chunks, SIDE, SIDE - 1)),
            dma, dma, dma((n_lat,)),
        ],
        compiler_params=pltpu.CompilerParams(
            collective_id=0, has_side_effects=True, dimension_semantics=("arbitrary",)
        ),
    )(transport, sigma_class, basin_id, depth_levels)
    kept = jax.ShapeDtypeStruct((BASINS, CLASSES, n_lat * LANES), jnp.bfloat16)
    return pl.pallas_call(
        keep_kernel,
        out_shape=kept,
        in_specs=[pl.BlockSpec(memory_space=pl.ANY)],
        out_specs=pl.BlockSpec(memory_space=pl.ANY),
        scratch_shapes=[pltpu.VMEM(kept.shape, kept.dtype), dma((BASINS,)), dma((BASINS,))],
    )(overturn.reshape(BASINS, HIGH * LOW, -1))


def solution(mesh):
    placed = (P(None, "lat", "lon"), P(None, "lat", "lon"), P("lat", "lon"), P("lat", "lon"))
    run = functools.partial(body, mesh.shape["lat"], mesh.shape["lon"])
    return jax.shard_map(run, mesh=mesh, in_specs=placed, out_specs=P(), check_vma=False)
```
